8 devices in a mesh: dp: 1 (over z), sp: 8 (over y, x, core).
Axes of the slice: x: 2, y: 2, z: 1, core: 2. Of those that a mesh axis runs over, the one named last changes fastest.
Arguments:
- hidden: bfloat16 [8192, 8192], P(('dp', 'sp'))
- grad_out: bfloat16 [8192, 8192], P(('dp', 'sp'))
- positions: int32 [8192], P(('dp', 'sp'))
- doc_ids: int32 [8192], P(('dp', 'sp'))
- w_q: bfloat16 [8192, 1024], replicated
- w_k: bfloat16 [8192, 128], replicated
- w_v: bfloat16 [8192, 128], replicated
- w_o: bfloat16 [1024, 8192], replicated
Outputs:
- output 1: bfloat16 [8192, 8192], P(('dp', 'sp'))
- output 2: bfloat16 [8192, 8192], P(('dp', 'sp'))
- output 3: float32 [8192, 1024], P('dp')
- output 4: float32 [8192, 128], P('dp')
- output 5: float32 [8192, 128], P('dp')
- output 6: float32 [1024, 8192], P('dp')
All inputs are finite; a program needn't handle non-finite values.
Results may differ from the reference program's by a relative error of at most 0.0117475.
Values are sent between devices in bfloat16 or wider.
A program may use at most 1 GiB of HBM per device.

```python
import jax
import jax.numpy as jnp
from jax import lax

D = 8192
HEADS = 8
KV_HEADS = 1
HEAD = 128
SEQ = 8192

ROPE_THETA = 500000.0
ROPE_FACTOR = 8.0
ROPE_LOW = 1.0
ROPE_HIGH = 4.0
ROPE_OLD_CTX = 8192.0
SCORE_LIMIT = 32 * 1024 * 1024
NEG_BIG = -1.0e30


def draw_layout(layout_key):
    cut_key, start_key = jax.random.split(layout_key)
    cut_points = jnp.sort(jax.random.randint(cut_key, (2,), SEQ // 8, SEQ - SEQ // 8))
    token_idx = jnp.arange(SEQ, dtype=jnp.int32)
    doc_ids = jnp.sum(token_idx[:, None] >= cut_points[None, :], axis=1).astype(jnp.int32)
    bounds = jnp.concatenate([jnp.zeros((1,), jnp.int32), cut_points.astype(jnp.int32)])
    starts = jax.random.randint(start_key, (3,), 0, SEQ)
    positions = (starts[doc_ids] + token_idx - bounds[doc_ids]).astype(jnp.int32)
    return positions, doc_ids


def setup_inputs(seed: int = 0, part: int = 0) -> dict:
    part_key = jax.random.fold_in(jax.random.key(seed), part)
    hid_key, grad_key, layout_key = jax.random.split(part_key, 3)
    weight_keys = jax.random.split(jax.random.key(seed + 1), 4)
    hidden = jax.random.normal(hid_key, (SEQ, D), jnp.float32).astype(jnp.bfloat16)
    grad_out = jax.random.normal(grad_key, (SEQ, D), jnp.float32).astype(jnp.bfloat16)
    positions, doc_ids = draw_layout(layout_key)
    in_scale = D ** -0.5
    w_q = (jax.random.normal(weight_keys[0], (D, HEADS * HEAD), jnp.float32) * in_scale).astype(jnp.bfloat16)
    w_k = (jax.random.normal(weight_keys[1], (D, KV_HEADS * HEAD), jnp.float32) * in_scale).astype(jnp.bfloat16)
    w_v = (jax.random.normal(weight_keys[2], (D, KV_HEADS * HEAD), jnp.float32) * in_scale).astype(jnp.bfloat16)
    w_o = (jax.random.normal(weight_keys[3], (HEADS * HEAD, D), jnp.float32) * (HEADS * HEAD) ** -0.5).astype(jnp.bfloat16)
    return {"hidden": hidden, "grad_out": grad_out, "positions": positions, "doc_ids": doc_ids, "w_q": w_q, "w_k": w_k, "w_v": w_v, "w_o": w_o}


def rope_freqs():
    half_idx = jnp.arange(HEAD // 2, dtype=jnp.float32)
    inv_freq = jnp.power(ROPE_THETA, -2.0 * half_idx / HEAD)
    wavelen = 2.0 * jnp.pi / inv_freq
    smooth = (ROPE_OLD_CTX / wavelen - ROPE_LOW) / (ROPE_HIGH - ROPE_LOW)
    mixed_freq = (1.0 - smooth) * inv_freq / ROPE_FACTOR + smooth * inv_freq
    scaled = jnp.where(wavelen > ROPE_OLD_CTX / ROPE_LOW, inv_freq / ROPE_FACTOR, mixed_freq)
    return jnp.where(wavelen < ROPE_OLD_CTX / ROPE_HIGH, inv_freq, scaled)


def rope_tables(pos_vec):
    angles = pos_vec.astype(jnp.float32)[:, None] * rope_freqs()[None, :]
    return jnp.cos(angles)[:, None, :], jnp.sin(angles)[:, None, :]


def rotate(values, cos_tab, sin_tab):
    half_dim = values.shape[-1] // 2
    first_half = values[..., :half_dim]
    second_half = values[..., half_dim:]
    return jnp.concatenate([first_half * cos_tab - second_half * sin_tab, second_half * cos_tab + first_half * sin_tab], axis=-1)


def block_rows(n_query, head_count, n_keys):
    block_len = n_query
    while block_len % 16 == 0 and head_count * block_len * n_keys > SCORE_LIMIT:
        block_len = block_len // 2
    return block_len


def block_probs(q_blk, k_all, pos_blk, doc_blk, pos_all, doc_all):
    scores = jnp.einsum("qhgd,shd->hgqs", q_blk, k_all) * HEAD ** -0.5
    allowed = (pos_all[None, :] <= pos_blk[:, None]) & (doc_all[None, :] == doc_blk[:, None])
    scores = jnp.where(allowed, scores, NEG_BIG)
    row_peak = jnp.max(scores, axis=-1, keepdims=True)
    exp_vals = jnp.exp(scores - row_peak)
    return exp_vals / jnp.sum(exp_vals, axis=-1, keepdims=True)


def reference(hidden, grad_out, positions, doc_ids, w_q, w_k, w_v, w_o):
    group_size = HEADS // KV_HEADS
    score_scale = HEAD ** -0.5
    cos_tab, sin_tab = rope_tables(positions)
    q_pre = jnp.dot(hidden, w_q, preferred_element_type=jnp.float32).reshape(SEQ, HEADS, HEAD)
    k_pre = jnp.dot(hidden, w_k, preferred_element_type=jnp.float32).reshape(SEQ, KV_HEADS, HEAD)
    v_pre = jnp.dot(hidden, w_v, preferred_element_type=jnp.float32).reshape(SEQ, KV_HEADS, HEAD)
    q_rot = rotate(q_pre, cos_tab, sin_tab).astype(jnp.bfloat16).astype(jnp.float32)
    k_rot = rotate(k_pre, cos_tab, sin_tab).astype(jnp.bfloat16).astype(jnp.float32)
    v_val = v_pre.astype(jnp.bfloat16).astype(jnp.float32)
    block_len = block_rows(SEQ, HEADS, SEQ)
    n_blocks = SEQ // block_len
    q_blocks = q_rot.reshape(n_blocks, block_len, KV_HEADS, group_size, HEAD)
    pos_blocks = positions.reshape(n_blocks, block_len)
    doc_blocks = doc_ids.reshape(n_blocks, block_len)

    def fwd_block(block_in):
        q_blk, pos_blk, doc_blk = block_in
        prob_f32 = block_probs(q_blk, k_rot, pos_blk, doc_blk, positions, doc_ids)
        prob_bf = prob_f32.astype(jnp.bfloat16).astype(jnp.float32)
        return jnp.einsum("hgqs,shd->qhgd", prob_bf, v_val).astype(jnp.bfloat16)

    context = lax.map(fwd_block, (q_blocks, pos_blocks, doc_blocks)).reshape(SEQ, HEADS * HEAD)
    attn_out = jnp.dot(context, w_o, preferred_element_type=jnp.float32).astype(jnp.bfloat16)

    d_ctx = jnp.dot(grad_out, w_o.T, preferred_element_type=jnp.float32).astype(jnp.bfloat16)
    grad_wo = jnp.dot(context.T, grad_out, preferred_element_type=jnp.float32)
    d_ctx_blocks = d_ctx.astype(jnp.float32).reshape(n_blocks, block_len, KV_HEADS, group_size, HEAD)

    def bwd_block(acc_pair, block_in):
        dk_acc, dv_acc = acc_pair
        q_blk, dctx_blk, pos_blk, doc_blk = block_in
        prob_f32 = block_probs(q_blk, k_rot, pos_blk, doc_blk, positions, doc_ids)
        prob_bf = prob_f32.astype(jnp.bfloat16).astype(jnp.float32)
        d_prob = jnp.einsum("qhgd,shd->hgqs", dctx_blk, v_val)
        row_dot = jnp.sum(prob_f32 * d_prob, axis=-1, keepdims=True)
        d_score = (prob_f32 * (d_prob - row_dot) * score_scale).astype(jnp.bfloat16).astype(jnp.float32)
        dq_blk = jnp.einsum("hgqs,shd->qhgd", d_score, k_rot).astype(jnp.bfloat16)
        dk_acc = dk_acc + jnp.einsum("hgqs,qhgd->shd", d_score, q_blk)
        dv_acc = dv_acc + jnp.einsum("hgqs,qhgd->shd", prob_bf, dctx_blk)
        return (dk_acc, dv_acc), dq_blk

    zero_acc = jnp.zeros((SEQ, KV_HEADS, HEAD), jnp.float32)
    (dk_acc, dv_acc), dq_blocks = lax.scan(bwd_block, (zero_acc, zero_acc), (q_blocks, d_ctx_blocks, pos_blocks, doc_blocks))
    dq_rot = dq_blocks.reshape(SEQ, HEADS, HEAD).astype(jnp.float32)
    dq_pre = rotate(dq_rot, cos_tab, -sin_tab).astype(jnp.bfloat16).reshape(SEQ, HEADS * HEAD)
    dk_rot = dk_acc.astype(jnp.bfloat16).astype(jnp.float32)
    dk_pre = rotate(dk_rot, cos_tab, -sin_tab).astype(jnp.bfloat16).reshape(SEQ, KV_HEADS * HEAD)
    dv_pre = dv_acc.astype(jnp.bfloat16).reshape(SEQ, KV_HEADS * HEAD)
    grad_hidden = (jnp.dot(dq_pre, w_q.T, preferred_element_type=jnp.float32) + jnp.dot(dk_pre, w_k.T, preferred_element_type=jnp.float32) + jnp.dot(dv_pre, w_v.T, preferred_element_type=jnp.float32)).astype(jnp.bfloat16)
    grad_wq = jnp.dot(hidden.T, dq_pre, preferred_element_type=jnp.float32)
    grad_wk = jnp.dot(hidden.T, dk_pre, preferred_element_type=jnp.float32)
    grad_wv = jnp.dot(hidden.T, dv_pre, preferred_element_type=jnp.float32)
    return attn_out, grad_hidden, grad_wq, grad_wk, grad_wv, grad_wo
```

```python
import functools

import jax
import jax.numpy as jnp
from jax import lax
from jax.experimental import pallas as pl
from jax.experimental.pallas import tpu as pltpu
from jax.sharding import PartitionSpec as P


HEAD_DIM = 128
ROPE_THETA = 500000.0
ROPE_FACTOR = 8.0
ROPE_LOW = 1.0
ROPE_HIGH = 4.0
ROPE_OLD_CTX = 8192.0
NEG_BIG = -1.0e30
LOG2E = 1.4426950408889634
SCALE = HEAD_DIM ** -0.5
KEY_BLOCK = 512
VMEM_LIMIT = 60 * 1024 * 1024


def all_gather(value):
    return lax.all_gather(value, "sp", tiled=True)


def reduce_scatter(value):
    return lax.psum_scatter(value, "sp", scatter_dimension=0, tiled=True)


def rope_freqs():
    half_idx = jnp.arange(HEAD_DIM // 2, dtype=jnp.float32)
    inv_freq = jnp.power(ROPE_THETA, -2.0 * half_idx / HEAD_DIM)
    wavelen = 2.0 * jnp.pi / inv_freq
    smooth = (ROPE_OLD_CTX / wavelen - ROPE_LOW) / (ROPE_HIGH - ROPE_LOW)
    mixed_freq = (1.0 - smooth) * inv_freq / ROPE_FACTOR + smooth * inv_freq
    scaled = jnp.where(wavelen > ROPE_OLD_CTX / ROPE_LOW, inv_freq / ROPE_FACTOR, mixed_freq)
    return jnp.where(wavelen < ROPE_OLD_CTX / ROPE_HIGH, inv_freq, scaled)


def rope_tables(pos_vec):
    angles = pos_vec.astype(jnp.float32)[:, None] * rope_freqs()[None, :]
    return jnp.cos(angles)[:, None, :], jnp.sin(angles)[:, None, :]


def rotate(values, cos_tab, sin_tab):
    half_dim = values.shape[-1] // 2
    first_half = values[..., :half_dim]
    second_half = values[..., half_dim:]
    return jnp.concatenate([first_half * cos_tab - second_half * sin_tab, second_half * cos_tab + first_half * sin_tab], axis=-1)


def dot_last(lhs_mat, rhs_mat):
    return lax.dot_general(lhs_mat, rhs_mat, (((1,), (1,)), ((), ())), preferred_element_type=jnp.float32)


def mm(lhs_mat, rhs_mat):
    return jnp.dot(lhs_mat, rhs_mat, preferred_element_type=jnp.float32)


def allowed_keys(block, tok, start):
    key = lax.broadcasted_iota(jnp.int32, (KEY_BLOCK, tok.shape[1]), 0) + block * KEY_BLOCK
    return (key >= start) & (key <= tok)


def fwd_kernel(n_heads, bounds, tok_ref, start_ref, q_ref, k_ref, v_ref, ctx_ref, lse_ref, qt, vt, acc, top, tot):
    tile = pl.program_id(0)
    tq = q_ref.shape[0]

    @pl.when(tile == 0)
    def _():
        def flip(i, c):
            rows = pl.ds(pl.multiple_of(i * KEY_BLOCK, KEY_BLOCK), KEY_BLOCK)
            vt[:, rows] = v_ref[rows, :].T
            return c

        lax.fori_loop(0, v_ref.shape[0] // KEY_BLOCK, flip, 0)

    for h in range(n_heads):
        qt[:, h * tq:(h + 1) * tq] = q_ref[:, h * HEAD_DIM:(h + 1) * HEAD_DIM].T
    acc[...] = jnp.zeros_like(acc)
    top[...] = jnp.full_like(top, NEG_BIG)
    tot[...] = jnp.zeros_like(tot)
    lo, full_lo, full_hi, hi = [bounds[4 * tile + i] for i in range(4)]

    def one_block(block, masked):
        rows = pl.ds(pl.multiple_of(block * KEY_BLOCK, KEY_BLOCK), KEY_BLOCK)
        keys = k_ref[rows, :]
        vals = vt[:, rows]
        keep = allowed_keys(block, tok_ref[0], start_ref[0]) if masked else None
        nxt = mm(keys, qt[:, 0:tq])
        for h in range(n_heads):
            cols = slice(h * tq, (h + 1) * tq)
            s = nxt
            if h + 1 < n_heads:
                nxt = mm(keys, qt[:, (h + 1) * tq:(h + 2) * tq])
            s = s * (SCALE * LOG2E)
            if masked:
                s = jnp.where(keep, s, NEG_BIG)
            old = top[:, cols]
            new = jnp.maximum(old, jnp.max(s, axis=0, keepdims=True))
            p = jnp.exp2(s - new)
            fade = jnp.exp2(old - new)
            top[:, cols] = new
            tot[:, cols] = tot[:, cols] * fade + jnp.sum(p, axis=0, keepdims=True)
            acc[:, cols] = acc[:, cols] * fade + mm(vals, p.astype(jnp.bfloat16))

    def step(block, c):
        inside = (block >= full_lo) & (block < full_hi)

        @pl.when(inside)
        def _():
            one_block(block, False)

        @pl.when(jnp.logical_not(inside))
        def _():
            one_block(block, True)

        return c

    lax.fori_loop(lo, hi, step, 0)
    for h in range(n_heads):
        cols = slice(h * tq, (h + 1) * tq)
        ctx_ref[:, h * HEAD_DIM:(h + 1) * HEAD_DIM] = (acc[:, cols] / tot[:, cols]).T.astype(jnp.bfloat16)
    lse_ref[0] = top[...] + jnp.log2(tot[...])


def bwd_kernel(n_heads, bounds, tok_ref, start_ref, lse_ref, q_ref, dctx_ref, ctx_ref, k_ref, v_ref, dq_ref, dkv_ref,
               qt, dt, kt, qrow, drow, pt, dst, dqt, delta):
    tile = pl.program_id(0)
    tq = q_ref.shape[0]

    @pl.when(tile == 0)
    def _():
        def flip(i, c):
            rows = pl.ds(pl.multiple_of(i * KEY_BLOCK, KEY_BLOCK), KEY_BLOCK)
            kt[:, rows] = k_ref[rows, :].T
            dkv_ref[rows, :] = jnp.zeros((KEY_BLOCK, 2 * HEAD_DIM), jnp.float32)
            return c

        lax.fori_loop(0, k_ref.shape[0] // KEY_BLOCK, flip, 0)

    for h in range(n_heads):
        cols = slice(h * tq, (h + 1) * tq)
        wide = slice(h * HEAD_DIM, (h + 1) * HEAD_DIM)
        q_h = q_ref[:, wide]
        d_h = dctx_ref[:, wide]
        qrow[cols, :] = q_h
        drow[cols, :] = d_h
        qt[:, cols] = q_h.T
        dt[:, cols] = d_h.T
        both = (ctx_ref[:, wide].astype(jnp.float32) * d_h.astype(jnp.float32)).T
        delta[:, cols] = jnp.sum(both, axis=0, keepdims=True)
    dqt[...] = jnp.zeros_like(dqt)
    lo, full_lo, full_hi, hi = [bounds[4 * tile + i] for i in range(4)]

    def one_block(block, masked):
        rows = pl.ds(pl.multiple_of(block * KEY_BLOCK, KEY_BLOCK), KEY_BLOCK)
        keys = k_ref[rows, :]
        vals = v_ref[rows, :]
        keep = allowed_keys(block, tok_ref[0], start_ref[0]) if masked else None
        for h in range(n_heads):
            cols = slice(h * tq, (h + 1) * tq)
            s = mm(keys, qt[:, cols])
            dp = mm(vals, dt[:, cols])
            p = jnp.exp2(s * (SCALE * LOG2E) - lse_ref[0, :, cols])
            if masked:
                p = jnp.where(keep, p, 0.0)
            pt[:, cols] = p.astype(jnp.bfloat16)
            dst[:, cols] = (p * (dp - delta[:, cols]) * SCALE).astype(jnp.bfloat16)
        dkv_ref[rows, HEAD_DIM:] += mm(pt[...], drow[...])
        dkv_ref[rows, :HEAD_DIM] += mm(dst[...], qrow[...])
        dqt[...] += mm(kt[:, rows], dst[...])

    def step(block, c):
        inside = (block >= full_lo) & (block < full_hi)

        @pl.when(inside)
        def _():
            one_block(block, False)

        @pl.when(jnp.logical_not(inside))
        def _():
            one_block(block, True)

        return c

    lax.fori_loop(lo, hi, step, 0)
    for h in range(n_heads):
        dq_ref[:, h * HEAD_DIM:(h + 1) * HEAD_DIM] = dqt[:, h * tq:(h + 1) * tq].T.astype(jnp.bfloat16)


def tile_specs(n_heads, tq, seq_len):
    row = pl.BlockSpec((1, 1, tq), lambda i, b: (i, 0, 0))
    stat = pl.BlockSpec((1, 1, n_heads * tq), lambda i, b: (i, 0, 0))
    tokens = pl.BlockSpec((tq, n_heads * HEAD_DIM), lambda i, b: (i, 0))
    whole = pl.BlockSpec((seq_len, HEAD_DIM), lambda i, b: (0, 0))
    return row, stat, tokens, whole


def attention_fwd(bounds, tok, start, q, k, v, tq):
    tokens, width = q.shape
    n_heads = width // HEAD_DIM
    seq_len = k.shape[0]
    n_tiles = tokens // tq
    row, stat, tile, whole = tile_specs(n_heads, tq, seq_len)
    m = n_heads * tq
    work = 4 * tokens * n_heads * HEAD_DIM * seq_len // 4
    return pl.pallas_call(
        functools.partial(fwd_kernel, n_heads),
        grid_spec=pltpu.PrefetchScalarGridSpec(
            num_scalar_prefetch=1,
            grid=(n_tiles,),
            in_specs=[row, row, tile, whole, whole],
            out_specs=[tile, stat],
            scratch_shapes=[
                pltpu.VMEM((HEAD_DIM, m), jnp.bfloat16),
                pltpu.VMEM((HEAD_DIM, seq_len), jnp.bfloat16),
                pltpu.VMEM((HEAD_DIM, m), jnp.float32),
                pltpu.VMEM((1, m), jnp.float32),
                pltpu.VMEM((1, m), jnp.float32),
            ],
        ),
        out_shape=[jax.ShapeDtypeStruct((tokens, width), jnp.bfloat16), jax.ShapeDtypeStruct((n_tiles, 1, m), jnp.float32)],
        compiler_params=pltpu.CompilerParams(dimension_semantics=("arbitrary",), vmem_limit_bytes=VMEM_LIMIT),
        cost_estimate=pl.CostEstimate(flops=work, bytes_accessed=16 * 1024 * 1024, transcendentals=work // 512),
        name="attn_fwd",
    )(bounds, tok, start, q, k, v)


def attention_bwd(bounds, tok, start, lse, q, dctx, ctx, k, v, tq):
    tokens, width = q.shape
    n_heads = width // HEAD_DIM
    seq_len = k.shape[0]
    n_tiles = tokens // tq
    row, stat, tile, whole = tile_specs(n_heads, tq, seq_len)
    m = n_heads * tq
    work = 10 * tokens * n_heads * HEAD_DIM * seq_len // 4
    return pl.pallas_call(
        functools.partial(bwd_kernel, n_heads),
        grid_spec=pltpu.PrefetchScalarGridSpec(
            num_scalar_prefetch=1,
            grid=(n_tiles,),
            in_specs=[row, row, stat, tile, tile, tile, whole, whole],
            out_specs=[tile, pl.BlockSpec((seq_len, 2 * HEAD_DIM), lambda i, b: (0, 0))],
            scratch_shapes=[
                pltpu.VMEM((HEAD_DIM, m), jnp.bfloat16),
                pltpu.VMEM((HEAD_DIM, m), jnp.bfloat16),
                pltpu.VMEM((HEAD_DIM, seq_len), jnp.bfloat16),
                pltpu.VMEM((m, HEAD_DIM), jnp.bfloat16),
                pltpu.VMEM((m, HEAD_DIM), jnp.bfloat16),
                pltpu.VMEM((KEY_BLOCK, m), jnp.bfloat16),
                pltpu.VMEM((KEY_BLOCK, m), jnp.bfloat16),
                pltpu.VMEM((HEAD_DIM, m), jnp.float32),
                pltpu.VMEM((1, m), jnp.float32),
            ],
        ),
        out_shape=[jax.ShapeDtypeStruct((tokens, width), jnp.bfloat16), jax.ShapeDtypeStruct((seq_len, 2 * HEAD_DIM), jnp.float32)],
        compiler_params=pltpu.CompilerParams(dimension_semantics=("arbitrary",), vmem_limit_bytes=VMEM_LIMIT),
        cost_estimate=pl.CostEstimate(flops=work, bytes_accessed=32 * 1024 * 1024, transcendentals=work // 1280),
        name="attn_bwd",
    )(bounds, tok, start, lse, q, dctx, ctx, k, v)


def outer_kernel(lhs_ref, rhs_ref, out_ref):
    out_ref[...] = lax.dot_general(lhs_ref[...], rhs_ref[...], (((0,), (0,)), ((), ())), preferred_element_type=jnp.float32)


def outer_rows(lhs_mat, rhs_mat, tile):
    tokens, rows = lhs_mat.shape
    cols = rhs_mat.shape[1]
    return pl.pallas_call(
        outer_kernel,
        grid=(rows // tile,),
        in_specs=[pl.BlockSpec((tokens, tile), lambda i: (0, i)), pl.BlockSpec((tokens, cols), lambda i: (0, 0))],
        out_specs=pl.BlockSpec((tile, cols), lambda i: (i, 0)),
        out_shape=jax.ShapeDtypeStruct((rows, cols), jnp.float32),
        compiler_params=pltpu.CompilerParams(dimension_semantics=("arbitrary",), vmem_limit_bytes=VMEM_LIMIT),
        cost_estimate=pl.CostEstimate(flops=2 * tokens * rows * cols, bytes_accessed=2 * tokens * (rows + cols) + 4 * rows * cols, transcendentals=0),
        name="outer_rows",
    )(lhs_mat, rhs_mat)


def outer_cols(lhs_mat, rhs_mat, tile):
    tokens, rows = lhs_mat.shape
    cols = rhs_mat.shape[1]
    return pl.pallas_call(
        outer_kernel,
        grid=(cols // tile,),
        in_specs=[pl.BlockSpec((tokens, rows), lambda i: (0, 0)), pl.BlockSpec((tokens, tile), lambda i: (0, i))],
        out_specs=pl.BlockSpec((rows, tile), lambda i: (0, i)),
        out_shape=jax.ShapeDtypeStruct((rows, cols), jnp.float32),
        compiler_params=pltpu.CompilerParams(dimension_semantics=("arbitrary",), vmem_limit_bytes=VMEM_LIMIT),
        cost_estimate=pl.CostEstimate(flops=2 * tokens * rows * cols, bytes_accessed=2 * tokens * (rows + cols) + 4 * rows * cols, transcendentals=0),
        name="outer_cols",
    )(lhs_mat, rhs_mat)


def key_bounds(start, tok, tq):
    first_tok, last_tok = tok[::tq], tok[tq - 1::tq]
    first_start, last_start = start[::tq], start[tq - 1::tq]
    lo = first_start // KEY_BLOCK
    hi = last_tok // KEY_BLOCK + 1
    full_lo = (last_start + KEY_BLOCK - 1) // KEY_BLOCK
    full_hi = (first_tok + 1) // KEY_BLOCK
    return jnp.stack([lo, full_lo, full_hi, hi], axis=1).reshape(-1)


def doc_bytes(doc_ids):
    parts = [(doc_ids >> (8 * i)) & 255 for i in range(4)]
    return jnp.concatenate([p.reshape(-1, 256) for p in parts], axis=0).astype(jnp.bfloat16)


def doc_words(rows):
    n = rows.shape[1] // 4
    ints = rows.astype(jnp.int32)
    parts = [ints[:, i * n:(i + 1) * n] << (8 * i) for i in range(4)]
    return (parts[0] | parts[1] | parts[2] | parts[3]).reshape(-1)


def solution(mesh):
    def layer(hidden, grad_out, positions, doc_ids, w_q, w_k, w_v, w_o):
        tokens = hidden.shape[0]
        num_q = w_q.shape[1] // HEAD_DIM
        me = lax.axis_index("sp")
        base = me * tokens
        tq = 128
        cos_tab, sin_tab = rope_tables(positions)

        kv_pre = mm(hidden, jnp.concatenate([w_k, w_v], axis=1))
        k_rot = rotate(kv_pre[:, :HEAD_DIM], cos_tab[:, 0], sin_tab[:, 0]).astype(jnp.bfloat16)
        kv = jnp.concatenate([k_rot, kv_pre[:, HEAD_DIM:].astype(jnp.bfloat16)], axis=1)
        packed = jnp.concatenate([kv, doc_bytes(doc_ids)], axis=0)
        gathered = lax.all_gather(packed, "sp")
        k_all = gathered[:, :tokens, :HEAD_DIM].reshape(-1, HEAD_DIM)
        v_all = gathered[:, :tokens, HEAD_DIM:].reshape(-1, HEAD_DIM)
        doc_all = doc_words(gathered[:, tokens:])

        q_pre = mm(hidden, w_q).reshape(tokens, -1, HEAD_DIM)
        q_rot = rotate(q_pre, cos_tab, sin_tab).astype(jnp.bfloat16).reshape(tokens, -1)

        inner = jnp.sum((doc_ids[None, :] < doc_ids[:, None]).astype(jnp.int32), axis=1)
        outer = jnp.sum((doc_all < doc_ids[0]).astype(jnp.int32))
        start = jnp.where(doc_ids == doc_ids[0], outer, base + inner)
        tok = base + jnp.arange(tokens, dtype=jnp.int32)
        bounds = key_bounds(start, tok, tq)
        tok_rows = tok.reshape(-1, 1, tq)
        start_rows = start.reshape(-1, 1, tq)

        ctx, lse = attention_fwd(bounds, tok_rows, start_rows, q_rot, k_all, v_all, tq)
        grad_wo = outer_cols(ctx, grad_out, 512)
        ctx, grad_wo = lax.optimization_barrier((ctx, grad_wo))
        grad_wo = reduce_scatter(grad_wo)
        grad_wo = all_gather(grad_wo)
        attn_out = mm(ctx, w_o).astype(jnp.bfloat16)
        d_ctx = dot_last(grad_out, w_o).astype(jnp.bfloat16)

        dq, dkv = attention_bwd(bounds, tok_rows, start_rows, lse, q_rot, d_ctx, ctx, k_all, v_all, tq)
        dkv = reduce_scatter(dkv)
        dq_pre = rotate(dq.reshape(tokens, num_q, HEAD_DIM).astype(jnp.float32), cos_tab, -sin_tab).astype(jnp.bfloat16).reshape(tokens, -1)
        grad_wq = outer_rows(hidden, dq_pre, 512)
        grad_wq = reduce_scatter(grad_wq)
        grad_wq = all_gather(grad_wq)

        dk_sum = dkv[:, :HEAD_DIM].astype(jnp.bfloat16).astype(jnp.float32)
        dk_pre = rotate(dk_sum, cos_tab[:, 0], -sin_tab[:, 0]).astype(jnp.bfloat16)
        dv_pre = dkv[:, HEAD_DIM:].astype(jnp.bfloat16)
        dkv_pre = jnp.concatenate([dk_pre, dv_pre], axis=1)
        grad_wkv = outer_rows(hidden, dkv_pre, 1024)
        grad_wkv = reduce_scatter(grad_wkv)
        grad_wkv = all_gather(grad_wkv)
        w_kv = jnp.concatenate([w_k, w_v], axis=1)
        grad_hidden = (dot_last(dq_pre, w_q) + dot_last(dkv_pre, w_kv)).astype(jnp.bfloat16)
        return attn_out, grad_hidden, grad_wq, grad_wkv[:, :HEAD_DIM], grad_wkv[:, HEAD_DIM:], grad_wo

    tok_spec = P(("dp", "sp"), None)
    vec_spec = P(("dp", "sp"))
    rep_spec = P(None, None)
    part_spec = P("dp", None)
    return jax.shard_map(layer, mesh=mesh, in_specs=(tok_spec, tok_spec, vec_spec, vec_spec, rep_spec, rep_spec, rep_spec, rep_spec), out_specs=(tok_spec, tok_spec, part_spec, part_spec, part_spec, part_spec), check_vma=False)
```

```python
import functools

import jax
import jax.numpy as jnp
from jax import lax
from jax.experimental import pallas as pl
from jax.experimental.pallas import tpu as pltpu
from jax.sharding import PartitionSpec as P


HEAD_DIM = 128
ROPE_THETA = 500000.0
ROPE_FACTOR = 8.0
ROPE_LOW = 1.0
ROPE_HIGH = 4.0
ROPE_OLD_CTX = 8192.0
NEG_BIG = -1.0e30
LOG2E = 1.4426950408889634
SCALE = HEAD_DIM ** -0.5
EXP2_SCALE = SCALE * LOG2E
KEY_BLOCK = 512
VMEM_LIMIT = 60 * 1024 * 1024
MESH = pl.DeviceIdType.MESH


def rope_freqs():
    half_idx = jnp.arange(HEAD_DIM // 2, dtype=jnp.float32)
    inv_freq = jnp.power(ROPE_THETA, -2.0 * half_idx / HEAD_DIM)
    wavelen = 2.0 * jnp.pi / inv_freq
    smooth = (ROPE_OLD_CTX / wavelen - ROPE_LOW) / (ROPE_HIGH - ROPE_LOW)
    mixed_freq = (1.0 - smooth) * inv_freq / ROPE_FACTOR + smooth * inv_freq
    scaled = jnp.where(wavelen > ROPE_OLD_CTX / ROPE_LOW, inv_freq / ROPE_FACTOR, mixed_freq)
    return jnp.where(wavelen < ROPE_OLD_CTX / ROPE_HIGH, inv_freq, scaled)


def rope_tables(pos_vec):
    angles = pos_vec.astype(jnp.float32)[:, None] * rope_freqs()[None, :]
    cos_tab, sin_tab = jnp.cos(angles), jnp.sin(angles)
    return jnp.concatenate([cos_tab, cos_tab], axis=1), jnp.concatenate([-sin_tab, sin_tab], axis=1)


def rotate(values, cos_tab, sin_tab):
    half_dim = values.shape[-1] // 2
    swapped = jnp.concatenate([values[:, half_dim:], values[:, :half_dim]], axis=1)
    return values * cos_tab + swapped * sin_tab


def spin(values, cos_tab, sin_tab):
    return values * cos_tab + pltpu.roll(values, HEAD_DIM // 2, 1) * sin_tab


def dot_last(lhs_mat, rhs_mat):
    return lax.dot_general(lhs_mat, rhs_mat, (((1,), (1,)), ((), ())), preferred_element_type=jnp.float32)


def mm(lhs_mat, rhs_mat):
    return jnp.dot(lhs_mat, rhs_mat, preferred_element_type=jnp.float32)


def places():
    me = lax.axis_index("sp")
    core = me % 2
    mate = me + 1 - 2 * core
    across = me + 2 - 4 * ((me // 2) % 2)
    along = me + 4 - 8 * (me // 4)
    return me, core, mate, across, along


def document_starts(docs):
    rows, lanes = docs.shape
    row = lax.broadcasted_iota(jnp.int32, docs.shape, 0)
    lane = lax.broadcasted_iota(jnp.int32, docs.shape, 1)
    index = row * lanes + lane
    before = pltpu.roll(docs, 1, 1)
    before = jnp.where(lane == 0, pltpu.roll(before, 1, 0), before)
    best = jnp.where((docs != before) | (index == 0), index, 0)
    shift = 1
    while shift < lanes:
        best = jnp.maximum(best, jnp.where(lane >= shift, pltpu.roll(best, shift, 1), 0))
        shift *= 2
    above = jnp.broadcast_to(best[:, lanes - 1:], docs.shape)
    shift = 1
    while shift < rows:
        above = jnp.maximum(above, jnp.where(row >= shift, pltpu.roll(above, shift, 0), 0))
        shift *= 2
    return jnp.maximum(best, jnp.where(row >= 1, pltpu.roll(above, 1, 0), 0))


def project_kernel(x_hbm, wk_hbm, wv_hbm, wq_hbm, cos_ref, sin_ref, doc_ref, kv_out, q_out, start_ref,
                   xv, wkv, wqv, acc, kvb, qb, docs, load_sem, wq_sem, keep_sem, send_sem, recv_sem, doc_send, doc_recv):
    me, core, mate, across, along = places()
    _, depth = xv.shape
    n_chunks = load_sem.shape[0] // 3
    chunk = depth // n_chunks
    n_tiles = qb.shape[0]
    rows = kvb.shape[0]
    half = rows // 2
    n_devices = kv_out.shape[0]
    doc_rows = doc_ref.shape[0]
    barrier = pltpu.get_barrier_semaphore()
    for k in range(1, n_devices):
        pl.semaphore_signal(barrier, inc=1, device_id={"sp": (me + k) % n_devices}, device_id_type=MESH)

    def loads(c):
        part = pl.ds(pl.multiple_of(c * chunk, chunk), chunk)
        return (
            pltpu.make_async_copy(x_hbm.at[:, part], xv.at[:, part], load_sem.at[3 * c]),
            pltpu.make_async_copy(wk_hbm.at[part, :], wkv.at[part, 0:HEAD_DIM], load_sem.at[3 * c + 1]),
            pltpu.make_async_copy(wv_hbm.at[part, :], wkv.at[part, HEAD_DIM:], load_sem.at[3 * c + 2]),
        )

    def load_wq(n):
        cols = pl.ds(pl.multiple_of(n * 2 * HEAD_DIM, 2 * HEAD_DIM), 2 * HEAD_DIM)
        return pltpu.make_async_copy(wq_hbm.at[:, cols], wqv.at[n % 2], wq_sem.at[n % 2])

    def send(src, dst, slot, peer):
        return pltpu.make_async_remote_copy(src_ref=src, dst_ref=dst, send_sem=send_sem.at[slot], recv_sem=recv_sem.at[slot], device_id={"sp": peer}, device_id_type=MESH)

    for c in range(n_chunks):
        for copy in loads(c):
            copy.start()
    load_wq(0).start()
    load_wq(1).start()

    docs[pl.ds(pl.multiple_of(me * doc_rows, doc_rows), doc_rows), :] = doc_ref[...]
    acc[...] = jnp.zeros_like(acc)
    pl.semaphore_wait(barrier, n_devices - 1)

    def tell(k, owner):
        at = docs.at[pl.ds(pl.multiple_of(owner * doc_rows, doc_rows), doc_rows), :]
        return pltpu.make_async_remote_copy(src_ref=doc_ref, dst_ref=at, send_sem=doc_send.at[k - 1], recv_sem=doc_recv.at[k - 1], device_id={"sp": (me + k) % n_devices}, device_id_type=MESH)

    for k in range(1, n_devices):
        tell(k, me).start()

    def kv_step(c, carry):
        for copy in loads(c):
            copy.wait()
        part = pl.ds(pl.multiple_of(c * chunk, chunk), chunk)
        acc[...] += mm(xv[:, part], wkv[part, :])
        return carry

    lax.fori_loop(0, n_chunks, kv_step, 0)
    kvb[:, 0:HEAD_DIM] = spin(acc[:, 0:HEAD_DIM], cos_ref[...], sin_ref[...]).astype(jnp.bfloat16)
    kvb[:, HEAD_DIM:] = acc[:, HEAD_DIM:].astype(jnp.bfloat16)

    low, high = pl.ds(0, half), pl.ds(half, rows - half)
    far = along + (across - me)
    keep = pltpu.make_async_copy(kvb, kv_out.at[me], keep_sem.at[0])
    own = [send(kvb, kv_out.at[me], slot, peer) for slot, peer in ((0, across), (1, along), (2, mate))]
    keep.start()
    for copy in own:
        copy.start()
    fwd = [
        send(kv_out.at[along, low], kv_out.at[along, low], 3, across),
        send(kv_out.at[across, high], kv_out.at[across, high], 4, along),
        send(kv_out.at[across], kv_out.at[across], 5, mate),
        send(kv_out.at[along], kv_out.at[along], 6, mate),
    ]
    last = [
        send(kv_out.at[far, low], kv_out.at[far, low], 7, mate),
        send(kv_out.at[far, high], kv_out.at[far, high], 8, mate),
    ]

    def mate_of(device):
        return device + 1 - 2 * (device % 2)

    def arrive(dst, slot):
        return send(dst, dst, slot, me)

    def keep_q(n):
        return pltpu.make_async_copy(qb.at[n], q_out.at[0, n % 2], keep_sem.at[1 + n % 2])

    def give_q(n):
        return send(qb.at[n], q_out.at[1, n % 2], 9 + n % 2, mate)

    def q_step(n, carry):
        load_wq(n).wait()
        y = mm(xv[...], wqv[n % 2])
        for h in range(2):
            wide = slice(h * HEAD_DIM, (h + 1) * HEAD_DIM)
            qb[n, :, wide] = spin(y[:, wide], cos_ref[...], sin_ref[...]).astype(jnp.bfloat16)

        @pl.when(n + 2 < n_tiles)
        def _():
            load_wq(n + 2).start()

        @pl.when(n // 2 == core)
        def _():
            keep_q(n).start()

        @pl.when(n // 2 != core)
        def _():
            give_q(n).start()

        @pl.when(n == n_tiles - 2)
        def _():
            arrive(kv_out.at[across], 0).wait_recv()
            arrive(kv_out.at[along], 1).wait_recv()
            for copy in fwd:
                copy.start()

        return carry

    lax.fori_loop(0, n_tiles, q_step, 0)
    arrive(kv_out.at[far, low], 3).wait_recv()
    arrive(kv_out.at[far, high], 4).wait_recv()
    for copy in last:
        copy.start()
    keep.wait()
    for t in range(2):
        keep_q(2 * core + t).wait()
        give_q(2 * (1 - core) + t).wait_send()
        arrive(q_out.at[1, t], 9 + t).wait_recv()
    arrive(kv_out.at[mate], 2).wait_recv()
    arrive(kv_out.at[mate_of(across)], 5).wait_recv()
    arrive(kv_out.at[mate_of(along)], 6).wait_recv()
    arrive(kv_out.at[mate_of(far), low], 7).wait_recv()
    arrive(kv_out.at[mate_of(far), high], 8).wait_recv()
    for copy in own + fwd + last:
        copy.wait_send()
    for k in range(1, n_devices):
        tell(k, me).wait_send()
        tell(k, (me + n_devices - k) % n_devices).wait_recv()
    start_ref[...] = document_starts(docs[...])


def project(hidden, w_q, w_k, w_v, cos_tab, sin_tab, doc_ids, n_devices):
    tokens, depth = hidden.shape
    width = w_q.shape[1]
    n_tiles = width // (2 * HEAD_DIM)
    n_chunks = 4
    doc_shape = (tokens // 128, 128)
    hbm = pl.BlockSpec(memory_space=pl.ANY)
    vmem = pl.BlockSpec(memory_space=pltpu.VMEM)
    return pl.pallas_call(
        project_kernel,
        in_specs=[hbm, hbm, hbm, hbm, vmem, vmem, vmem],
        out_specs=[hbm, hbm, vmem],
        out_shape=[
            jax.ShapeDtypeStruct((n_devices, tokens, 2 * HEAD_DIM), jnp.bfloat16),
            jax.ShapeDtypeStruct((2, n_tiles // 2, tokens, 2 * HEAD_DIM), jnp.bfloat16),
            jax.ShapeDtypeStruct((n_devices * doc_shape[0], doc_shape[1]), jnp.int32),
        ],
        scratch_shapes=[
            pltpu.VMEM((tokens, depth), jnp.bfloat16),
            pltpu.VMEM((depth, 2 * HEAD_DIM), jnp.bfloat16),
            pltpu.VMEM((2, depth, 2 * HEAD_DIM), jnp.bfloat16),
            pltpu.VMEM((tokens, 2 * HEAD_DIM), jnp.float32),
            pltpu.VMEM((tokens, 2 * HEAD_DIM), jnp.bfloat16),
            pltpu.VMEM((n_tiles, tokens, 2 * HEAD_DIM), jnp.bfloat16),
            pltpu.VMEM((n_devices * doc_shape[0], doc_shape[1]), jnp.int32),
            pltpu.SemaphoreType.DMA((3 * n_chunks,)),
            pltpu.SemaphoreType.DMA((2,)),
            pltpu.SemaphoreType.DMA((3,)),
            pltpu.SemaphoreType.DMA((11,)),
            pltpu.SemaphoreType.DMA((11,)),
            pltpu.SemaphoreType.DMA((n_devices - 1,)),
            pltpu.SemaphoreType.DMA((n_devices - 1,)),
        ],
        compiler_params=pltpu.CompilerParams(collective_id=0, has_side_effects=True, vmem_limit_bytes=VMEM_LIMIT),
        cost_estimate=pl.CostEstimate(flops=2 * tokens * depth * (width + 2 * HEAD_DIM), bytes_accessed=2 * depth * (tokens + width), transcendentals=0),
        name="project",
    )(hidden, w_k, w_v, w_q, cos_tab, sin_tab, doc_ids.reshape(doc_shape))


def key_rows(block):
    return pl.ds(pl.multiple_of(block * KEY_BLOCK, KEY_BLOCK), KEY_BLOCK)


def tile_range(start_smem, tq):
    tile = pl.program_id(0)
    half_tiles = pl.num_programs(0) // 2
    me, _, mate, _, _ = places()
    first_tok = (jnp.where(tile < half_tiles, me, mate) * half_tiles + tile % half_tiles) * tq
    first_start = start_smem[first_tok]
    last_start = start_smem[first_tok + tq - 1]
    lo = first_start // KEY_BLOCK
    hi = (first_tok + tq - 1) // KEY_BLOCK + 1
    full_lo = (last_start + KEY_BLOCK - 1) // KEY_BLOCK
    full_hi = (first_tok + 1) // KEY_BLOCK
    return first_tok, lo, full_lo, full_hi, hi


def start_row(start_ref, first_tok, tq):
    lanes = start_ref.shape[1]
    return jnp.concatenate([start_ref[pl.ds(first_tok // lanes + i, 1), :] for i in range(tq // lanes)], axis=1)


def allowed_keys(block, first_tok, start):
    shape = (KEY_BLOCK, start.shape[1])
    key = lax.broadcasted_iota(jnp.int32, shape, 0) + block * KEY_BLOCK
    tok = lax.broadcasted_iota(jnp.int32, shape, 1) + first_tok
    return (key >= start) & (key <= tok)


def for_blocks(one_block, lo, full_lo, full_hi, hi):
    def step(block, c):
        inside = (block >= full_lo) & (block < full_hi)

        @pl.when(inside)
        def _():
            one_block(block, False)

        @pl.when(jnp.logical_not(inside))
        def _():
            one_block(block, True)

        return c

    lax.fori_loop(lo, hi, step, 0)


def fwd_kernel(start_smem, start_ref, q_ref, kv_ref, ctx_ref, lse_ref, qt, vt, acc, top, tot):
    tile = pl.program_id(0)
    tq = q_ref.shape[2]
    n_heads = 2 * q_ref.shape[1]

    @pl.when(tile == 0)
    def _():
        def flip(i, c):
            vt[:, key_rows(i)] = kv_ref[key_rows(i), HEAD_DIM:].T
            return c

        lax.fori_loop(0, vt.shape[1] // KEY_BLOCK, flip, 0)

    for h in range(n_heads):
        qt[:, h * tq:(h + 1) * tq] = q_ref[0, h // 2, :, (h % 2) * HEAD_DIM:(h % 2 + 1) * HEAD_DIM].T
    acc[...] = jnp.zeros_like(acc)
    top[...] = jnp.full_like(top, NEG_BIG)
    tot[...] = jnp.zeros_like(tot)
    first_tok, lo, full_lo, full_hi, hi = tile_range(start_smem, tq)

    def one_block(block, masked):
        keys = kv_ref[key_rows(block), :HEAD_DIM]
        vals = vt[:, key_rows(block)]
        keep = allowed_keys(block, first_tok, start_row(start_ref, first_tok, tq)) if masked else None
        nxt = mm(keys, qt[:, 0:tq])
        for h in range(n_heads):
            cols = slice(h * tq, (h + 1) * tq)
            s = nxt
            if h + 1 < n_heads:
                nxt = mm(keys, qt[:, (h + 1) * tq:(h + 2) * tq])
            if masked:
                s = jnp.where(keep, s, NEG_BIG)
            old = top[:, cols]
            new = jnp.maximum(old, jnp.max(s, axis=0, keepdims=True))
            base = new * EXP2_SCALE
            p = jnp.exp2(s * EXP2_SCALE - base)
            fade = jnp.exp2(old * EXP2_SCALE - base)
            top[:, cols] = new
            tot[:, cols] = tot[:, cols] * fade + jnp.sum(p, axis=0, keepdims=True)
            acc[:, cols] = acc[:, cols] * fade + mm(vals, p.astype(jnp.bfloat16))

    for_blocks(one_block, lo, full_lo, full_hi, hi)
    for h in range(n_heads):
        cols = slice(h * tq, (h + 1) * tq)
        ctx_ref[0, :, h * HEAD_DIM:(h + 1) * HEAD_DIM] = (acc[:, cols] / tot[:, cols]).T.astype(jnp.bfloat16)
    lse_ref[0] = top[...] * EXP2_SCALE + jnp.log2(tot[...])


def bwd_kernel(start_smem, start_ref, lse_ref, q_ref, dctx_ref, ctx_ref, cos_ref, sin_ref, kv_ref, dq_ref, dkv_ref,
               qt, dt, kt, qrow, drow, pt, dst, dqt, delta):
    tile = pl.program_id(0)
    tq = q_ref.shape[2]
    n_heads = 2 * q_ref.shape[1]

    @pl.when(tile == 0)
    def _():
        def flip(i, c):
            rows = key_rows(i)
            kt[:, rows] = kv_ref[rows, :HEAD_DIM].T
            dkv_ref[rows, :] = jnp.zeros((KEY_BLOCK, 2 * HEAD_DIM), jnp.float32)
            return c

        lax.fori_loop(0, kt.shape[1] // KEY_BLOCK, flip, 0)

    for h in range(n_heads):
        cols = slice(h * tq, (h + 1) * tq)
        wide = slice(h * HEAD_DIM, (h + 1) * HEAD_DIM)
        q_h = q_ref[0, h // 2, :, (h % 2) * HEAD_DIM:(h % 2 + 1) * HEAD_DIM]
        d_h = dctx_ref[0, :, wide]
        qrow[cols, :] = q_h
        drow[cols, :] = d_h
        qt[:, cols] = q_h.T
        dt[:, cols] = d_h.T
        both = (ctx_ref[0, :, wide].astype(jnp.float32) * d_h.astype(jnp.float32)).T
        delta[:, cols] = jnp.sum(both, axis=0, keepdims=True)
    dqt[...] = jnp.zeros_like(dqt)
    first_tok, lo, full_lo, full_hi, hi = tile_range(start_smem, tq)

    def one_block(block, masked):
        rows = key_rows(block)
        keys = kv_ref[rows, :HEAD_DIM]
        vals = kv_ref[rows, HEAD_DIM:]
        keep = allowed_keys(block, first_tok, start_row(start_ref, first_tok, tq)) if masked else None
        for h in range(n_heads):
            cols = slice(h * tq, (h + 1) * tq)
            s = mm(keys, qt[:, cols])
            dp = mm(vals, dt[:, cols])
            p = jnp.exp2(s * EXP2_SCALE - lse_ref[0, :, cols])
            if masked:
                p = jnp.where(keep, p, 0.0)
            pt[:, cols] = p.astype(jnp.bfloat16)
            dst[:, cols] = (p * (dp - delta[:, cols]) * SCALE).astype(jnp.bfloat16)
        dkv_ref[rows, HEAD_DIM:] += mm(pt[...], drow[...])
        dkv_ref[rows, :HEAD_DIM] += mm(dst[...], qrow[...])
        dqt[...] += mm(kt[:, rows], dst[...])

    for_blocks(one_block, lo, full_lo, full_hi, hi)
    for h in range(n_heads):
        dq = dqt[:, h * tq:(h + 1) * tq].T.astype(jnp.bfloat16).astype(jnp.float32)
        dq_ref[0, :, h * HEAD_DIM:(h + 1) * HEAD_DIM] = spin(dq, cos_ref[0], -sin_ref[0]).astype(jnp.bfloat16)


def attention_specs(tq, half_tiles, n_heads, kv_rows):
    start = pl.BlockSpec((kv_rows // 128, 128), lambda i, b: (0, 0))
    stat = pl.BlockSpec((1, 1, n_heads * tq), lambda i, b: (i, 0, 0))
    pairs = pl.BlockSpec((1, n_heads // 2, tq, 2 * HEAD_DIM), lambda i, b: (i // half_tiles, 0, i % half_tiles, 0))
    wide = pl.BlockSpec((1, tq, n_heads * HEAD_DIM), lambda i, b: (i // half_tiles, i % half_tiles, 0))
    table = pl.BlockSpec((1, tq, HEAD_DIM), lambda i, b: (i // half_tiles, i % half_tiles, 0))
    kv = pl.BlockSpec((kv_rows, 2 * HEAD_DIM), lambda i, b: (0, 0))
    return start, stat, pairs, wide, table, kv


def attention_fwd(start, q, kv, tq):
    _, n_pairs, tokens, _ = q.shape
    n_heads = 2 * n_pairs
    half_tiles = tokens // tq
    seq_len = kv.shape[0] * tokens
    kv = kv.reshape(-1, 2 * HEAD_DIM)
    start_spec, stat, pairs, wide, _, kv_spec = attention_specs(tq, half_tiles, n_heads, kv.shape[0])
    m = n_heads * tq
    work = 8 * tokens * n_heads * HEAD_DIM * seq_len // 4
    return pl.pallas_call(
        fwd_kernel,
        grid_spec=pltpu.PrefetchScalarGridSpec(
            num_scalar_prefetch=1,
            grid=(2 * half_tiles,),
            in_specs=[start_spec, pairs, kv_spec],
            out_specs=[wide, stat],
            scratch_shapes=[
                pltpu.VMEM((HEAD_DIM, m), jnp.bfloat16),
                pltpu.VMEM((HEAD_DIM, seq_len), jnp.bfloat16),
                pltpu.VMEM((HEAD_DIM, m), jnp.float32),
                pltpu.VMEM((1, m), jnp.float32),
                pltpu.VMEM((1, m), jnp.float32),
            ],
        ),
        out_shape=[jax.ShapeDtypeStruct((2, tokens, n_heads * HEAD_DIM), jnp.bfloat16), jax.ShapeDtypeStruct((2 * half_tiles, 1, m), jnp.float32)],
        compiler_params=pltpu.CompilerParams(dimension_semantics=("arbitrary",), vmem_limit_bytes=VMEM_LIMIT),
        cost_estimate=pl.CostEstimate(flops=work, bytes_accessed=16 * 1024 * 1024, transcendentals=work // 512),
        name="attn_fwd",
    )(start.reshape(-1), start, q, kv)


def attention_bwd(start, lse, q, dctx, ctx, cos2, sin2, kv, tq):
    _, n_pairs, tokens, _ = q.shape
    n_heads = 2 * n_pairs
    half_tiles = tokens // tq
    seq_len = kv.shape[0] * tokens
    kv = kv.reshape(-1, 2 * HEAD_DIM)
    start_spec, stat, pairs, wide, table, kv_spec = attention_specs(tq, half_tiles, n_heads, kv.shape[0])
    m = n_heads * tq
    work = 20 * tokens * n_heads * HEAD_DIM * seq_len // 4
    return pl.pallas_call(
        bwd_kernel,
        grid_spec=pltpu.PrefetchScalarGridSpec(
            num_scalar_prefetch=1,
            grid=(2 * half_tiles,),
            in_specs=[start_spec, stat, pairs, wide, wide, table, table, kv_spec],
            out_specs=[wide, pl.BlockSpec((seq_len, 2 * HEAD_DIM), lambda i, b: (0, 0))],
            scratch_shapes=[
                pltpu.VMEM((HEAD_DIM, m), jnp.bfloat16),
                pltpu.VMEM((HEAD_DIM, m), jnp.bfloat16),
                pltpu.VMEM((HEAD_DIM, seq_len), jnp.bfloat16),
                pltpu.VMEM((m, HEAD_DIM), jnp.bfloat16),
                pltpu.VMEM((m, HEAD_DIM), jnp.bfloat16),
                pltpu.VMEM((KEY_BLOCK, m), jnp.bfloat16),
                pltpu.VMEM((KEY_BLOCK, m), jnp.bfloat16),
                pltpu.VMEM((HEAD_DIM, m), jnp.float32),
                pltpu.VMEM((1, m), jnp.float32),
            ],
        ),
        out_shape=[jax.ShapeDtypeStruct((2, tokens, n_heads * HEAD_DIM), jnp.bfloat16), jax.ShapeDtypeStruct((seq_len, 2 * HEAD_DIM), jnp.float32)],
        compiler_params=pltpu.CompilerParams(dimension_semantics=("arbitrary",), vmem_limit_bytes=VMEM_LIMIT),
        cost_estimate=pl.CostEstimate(flops=work, bytes_accessed=32 * 1024 * 1024, transcendentals=work // 1280),
        name="attn_bwd",
    )(start.reshape(-1), start, lse, q, dctx, ctx, cos2, sin2, kv)


def wo_kernel(ctx_ref, own_ref, other_ref, out_ref, ctx_t):
    tokens = ctx_ref.shape[1]

    @pl.when(pl.program_id(0) == 0)
    def _():
        for part in range(2):
            ctx_t[:, part * tokens:(part + 1) * tokens] = ctx_ref[part].T

    out_ref[...] = mm(ctx_t[:, :tokens], own_ref[...]) + mm(ctx_t[:, tokens:], other_ref[...])


def outer_wo(ctx, own, other, tile):
    _, tokens, rows = ctx.shape
    cols = own.shape[1]
    step = pl.BlockSpec((tokens, tile), lambda i: (0, i))
    return pl.pallas_call(
        wo_kernel,
        grid=(cols // tile,),
        in_specs=[pl.BlockSpec((2, tokens, rows), lambda i: (0, 0, 0)), step, step],
        out_specs=pl.BlockSpec((rows, tile), lambda i: (0, i)),
        out_shape=jax.ShapeDtypeStruct((rows, cols), jnp.float32),
        scratch_shapes=[pltpu.VMEM((rows, 2 * tokens), jnp.bfloat16)],
        compiler_params=pltpu.CompilerParams(dimension_semantics=("arbitrary",), vmem_limit_bytes=VMEM_LIMIT),
        cost_estimate=pl.CostEstimate(flops=4 * tokens * rows * cols, bytes_accessed=4 * tokens * cols + 4 * rows * cols, transcendentals=0),
        name="outer_wo",
    )(ctx, own, other)


def outer_kernel(n_parts, *refs):
    out_ref = refs[-1]
    total = None
    for part in range(n_parts):
        rhs = refs[n_parts][part]
        term = mm(refs[part][...].T, rhs)
        total = term if total is None else total + term
    out_ref[...] = total


def outer_rows(lhs_parts, rhs, tile):
    n_parts, tokens, cols = rhs.shape
    rows = lhs_parts[0].shape[1]
    return pl.pallas_call(
        functools.partial(outer_kernel, n_parts),
        grid=(rows // tile,),
        in_specs=[pl.BlockSpec((tokens, tile), lambda i: (0, i))] * n_parts + [pl.BlockSpec((n_parts, tokens, cols), lambda i: (0, 0, 0))],
        out_specs=pl.BlockSpec((tile, cols), lambda i: (i, 0)),
        out_shape=jax.ShapeDtypeStruct((rows, cols), jnp.float32),
        compiler_params=pltpu.CompilerParams(dimension_semantics=("arbitrary",), vmem_limit_bytes=VMEM_LIMIT),
        cost_estimate=pl.CostEstimate(flops=2 * n_parts * tokens * rows * cols, bytes_accessed=2 * n_parts * tokens * (rows + cols) + 4 * rows * cols, transcendentals=0),
        name="outer_rows",
    )(*lhs_parts, rhs)


def copy_kernel(src_ref, dst_ref):
    dst_ref[...] = src_ref[...]


def place_wo(parts):
    n, rows, cols = parts.shape
    return pl.pallas_call(
        lambda src_ref, dst_ref: copy_kernel(src_ref.at[0], dst_ref),
        grid=(n, 2),
        in_specs=[pl.BlockSpec((1, rows // 2, cols), lambda i, r: (2 * (i % (n // 2)) + i // (n // 2), r, 0))],
        out_specs=pl.BlockSpec((rows // 2, cols), lambda i, r: (2 * i + r, 0)),
        out_shape=jax.ShapeDtypeStruct((n * rows, cols), parts.dtype),
        compiler_params=pltpu.CompilerParams(dimension_semantics=("arbitrary", "arbitrary"), vmem_limit_bytes=VMEM_LIMIT),
        cost_estimate=pl.CostEstimate(flops=10 ** 9, bytes_accessed=8 * n * rows * cols, transcendentals=0),
        name="place_wo",
    )(parts)


def place_wq(parts):
    n, rows, cols = parts.shape
    split = 2
    return pl.pallas_call(
        lambda src_ref, dst_ref: copy_kernel(src_ref.at[0], dst_ref),
        grid=(n, split),
        in_specs=[pl.BlockSpec((1, rows // split, cols), lambda i, r: (i, r, 0))],
        out_specs=pl.BlockSpec((rows // split, cols), lambda i, r: (i // 2 * split + r, i % 2)),
        out_shape=jax.ShapeDtypeStruct((n // 2 * rows, 2 * cols), parts.dtype),
        compiler_params=pltpu.CompilerParams(dimension_semantics=("arbitrary", "arbitrary"), vmem_limit_bytes=VMEM_LIMIT),
        cost_estimate=pl.CostEstimate(flops=10 ** 9, bytes_accessed=8 * n * rows * cols, transcendentals=0),
        name="place_wq",
    )(parts)


def split_kernel(src_ref, k_ref, v_ref):
    k_ref[...] = src_ref[:, :HEAD_DIM]
    v_ref[...] = src_ref[:, HEAD_DIM:]


def place_wkv(whole):
    rows, cols = whole.shape
    out = pl.BlockSpec((rows // 8, HEAD_DIM), lambda i: (i, 0))
    shape = jax.ShapeDtypeStruct((rows, HEAD_DIM), whole.dtype)
    return pl.pallas_call(
        split_kernel,
        grid=(8,),
        in_specs=[pl.BlockSpec((rows // 8, cols), lambda i: (i, 0))],
        out_specs=[out, out],
        out_shape=[shape, shape],
        compiler_params=pltpu.CompilerParams(dimension_semantics=("arbitrary",)),
        cost_estimate=pl.CostEstimate(flops=10 ** 8, bytes_accessed=8 * rows * cols, transcendentals=0),
        name="place_wkv",
    )(whole)


SAME_CORE = [[0, 2, 4, 6], [1, 3, 5, 7]]
SWAP = [(i, i + 1 - 2 * (i % 2)) for i in range(8)]


def swap(value):
    return lax.ppermute(value, "sp", SWAP)


def chip_scatter(value):
    return lax.psum_scatter(value, "sp", scatter_dimension=0, tiled=True, axis_index_groups=SAME_CORE)


def reduce_scatter(value):
    return lax.psum_scatter(value, "sp", scatter_dimension=0, tiled=True)


def all_gather(value):
    return lax.all_gather(value, "sp")


def solution(mesh):
    def layer(hidden, grad_out, positions, doc_ids, w_q, w_k, w_v, w_o):
        width = w_q.shape[1]
        tq = 256
        me = lax.axis_index("sp")
        core = me % 2
        first = core == 0

        def mine(value):
            return lax.dynamic_slice_in_dim(value, core * (width // 2), width // 2, axis=1)

        def others(value):
            return lax.dynamic_slice_in_dim(value, (1 - core) * (width // 2), width // 2, axis=1)

        def whole(own_half, other_half):
            return jnp.where(first, jnp.concatenate([own_half, other_half], axis=1), jnp.concatenate([other_half, own_half], axis=1))

        cos_tab, sin_tab = rope_tables(positions)
        kv, q, start = project(hidden, w_q, w_k, w_v, cos_tab, sin_tab, doc_ids, mesh.shape["sp"])

        ctx, lse = attention_fwd(start, q, kv, tq)
        other_grad = swap(grad_out)
        wo_part = outer_wo(ctx, grad_out, other_grad, 512)
        ctx, wo_part = lax.optimization_barrier((ctx, wo_part))
        wo_own = chip_scatter(wo_part)
        wo_all = all_gather(wo_own)

        d_ctx = dot_last(grad_out, w_o).astype(jnp.bfloat16)
        d_ctx2 = jnp.stack([mine(d_ctx), swap(others(d_ctx))])
        other_pos = swap(positions)
        cos_far, sin_far = rope_tables(other_pos)
        cos2, sin2 = jnp.stack([cos_tab, cos_far]), jnp.stack([sin_tab, sin_far])
        other_hidden = swap(hidden)

        ctx_rows = whole(ctx[0], swap(ctx[1]))
        attn_out = mm(ctx_rows, w_o).astype(jnp.bfloat16)

        dq, dkv = attention_bwd(start, lse, q, d_ctx2, ctx, cos2, sin2, kv, tq)
        wq_part = outer_rows((hidden, other_hidden), dq, 512)
        dkv_own = reduce_scatter(dkv)
        wq_own = chip_scatter(wq_part)
        wq_all = all_gather(wq_own)

        dk_sum = dkv_own[:, :HEAD_DIM].astype(jnp.bfloat16).astype(jnp.float32)
        dk_pre = rotate(dk_sum, cos_tab, -sin_tab).astype(jnp.bfloat16)
        dkv_pre = jnp.concatenate([dk_pre, dkv_own[:, HEAD_DIM:].astype(jnp.bfloat16)], axis=1)
        wkv_part = outer_rows((hidden,), dkv_pre[None], 1024)
        wkv_own = reduce_scatter(wkv_part)
        wkv_all = all_gather(wkv_own)
        dq_rows = whole(dq[0], swap(dq[1]))
        w_kv = jnp.concatenate([w_k, w_v], axis=1)
        grad_hidden = (dot_last(dq_rows, w_q) + dot_last(dkv_pre, w_kv)).astype(jnp.bfloat16)

        grad_wo = place_wo(wo_all)
        grad_wq = place_wq(wq_all)
        grad_wk, grad_wv = place_wkv(wkv_all.reshape(-1, 2 * HEAD_DIM))
        return attn_out, grad_hidden, grad_wq, grad_wk, grad_wv, grad_wo

    tok_spec = P(("dp", "sp"), None)
    vec_spec = P(("dp", "sp"))
    rep_spec = P(None, None)
    part_spec = P("dp", None)
    return jax.shard_map(layer, mesh=mesh, in_specs=(tok_spec, tok_spec, vec_spec, vec_spec, rep_spec, rep_spec, rep_spec, rep_spec), out_specs=(tok_spec, tok_spec, part_spec, part_spec, part_spec, part_spec), check_vma=False)
```
